32 devices in a mesh: parts: 2 (over x), inner: 16 (over z, y, core).
Axes of the slice: x: 2, y: 2, z: 4, core: 2. Of those that a mesh axis runs over, the one named last changes fastest.
Arguments:
- stem_slab: bfloat16 [2, 16384, 1024], P(None, ('parts', 'inner')), parts along dimension 1, may hold values from -6 to 6
- branches: bfloat16 [3, 2, 1024, 1024], P(None, None, 'inner'), may hold values from -0.1875 to 0.1875
- column_order: int32 [3, 1024], replicated, may hold values from 0 to 1023, each once within a row
Outputs:
- result_slab: bfloat16 [2, 16384, 1024], P(None, ('parts', 'inner')), parts along dimension 1
The draws below stay inside these ranges and needn't reach their ends.
There are 2 independent parts, one for each index of `parts`. The reference program is written for one: setup_inputs(seed, part) draws one part's arguments, and reference() takes and returns one part's arrays. A program takes and returns all parts, laid end to end along the dimension named above; an argument that names none is the same for every part. Nothing has to cross between parts.
Inputs may be any that keep to these rules, and one draw needn't show every extreme that they name: Each row of column_order names every number from 0 to 1023 exactly once.
All inputs are finite; a program needn't handle non-finite values.
Results may differ from the reference program's by a relative error of at most 0.0057.
Values may be sent and summed in bfloat16 or wider, within the bound.
No kernel may reach another device: no remote copies, remote signals or barrier semaphores. Data moves between devices by JAX's collectives and lax.ppermute only.
A program may use at most 64 MiB of HBM per device.

```python
import jax
import jax.numpy as jnp

BRANCH = 1024
ROWS_DEV = 512
STEPS = 3
ROWS = 8192
N_INNER = 16


def raised(array, key, source, target, blocks, factor):
    owner, partner = [(jnp.arange(array.shape[position]) // (array.shape[position] // blocks)).reshape([-1 if axis == position else 1 for axis in range(array.ndim)]) for position in (source, target)]
    chosen = jax.random.permutation(key, blocks)[partner]
    strong = (owner == chosen) | (owner == (partner + blocks // 2) % blocks)
    return jnp.where(strong, factor * array, array)


def block_scale(key, shape, pieces, least, top_value):
    loudness = 1.0
    for position, blocks in pieces:
        draws = jax.random.uniform(jax.random.fold_in(jax.random.fold_in(key, 6), position), (blocks,), jnp.float32, least / len(pieces), top_value / len(pieces))
        loudness = loudness * jnp.repeat(jnp.exp(draws), shape[position] // blocks).reshape((-1,) + (1,) * (len(shape) - 1 - position))
    return loudness


def noise(stream_key, extent, spread, limit, cuts=(), held_as=jnp.bfloat16):
    drawn = jax.random.normal(stream_key, extent, jnp.float32) * spread
    if len(cuts) > 0:
        drawn = block_scale(stream_key, extent, cuts, -0.22, 0.18) * drawn
    return jnp.clip(drawn, min=-limit, max=limit).astype(held_as)


def gaussian_with(own_key, extent, scale, most, cuts, heavy, kind=jnp.bfloat16):
    array = scale * jax.random.normal(own_key, extent, jnp.float32)
    if cuts:
        array = array * block_scale(own_key, extent, cuts, -0.22, 0.18)
    return jnp.clip(raised(array, jax.random.fold_in(own_key, 3), *heavy), -most, most).astype(kind)


def setup_inputs(seed: int = 0, part: int = 0) -> dict:
    key_list = jax.random.split(jax.random.key(seed), 4)
    own_keys = jax.random.split(jax.random.fold_in(key_list[3], part), 4)
    return {
        "stem_slab": noise(own_keys[0], (2, ROWS, BRANCH), 1.0, 6.0, ((1, 16),)),
        "branches": gaussian_with(key_list[1], (STEPS, 2, BRANCH, BRANCH), (2 * BRANCH) ** -0.5, 0.1875, ((2, 16),), (2, 3, 16, 2.0)),
        "column_order": jax.vmap(lambda own: jax.random.permutation(own, BRANCH))(jax.random.split(key_list[2], STEPS)).reshape((STEPS, BRANCH)).astype(jnp.int32),
    }


def contract(slab, order_row, pair):
    picked = jnp.take(slab, order_row.astype(jnp.int32), axis=2)
    real_part = jnp.dot(picked[0], pair[0], preferred_element_type=jnp.float32) - jnp.dot(picked[1], pair[1], preferred_element_type=jnp.float32)
    imag_part = jnp.dot(picked[0], pair[1], preferred_element_type=jnp.float32) + jnp.dot(picked[1], pair[0], preferred_element_type=jnp.float32)
    return jnp.stack([real_part, imag_part]).astype(jnp.bfloat16)


def swap_blocks(slab):
    width = BRANCH // N_INNER
    blocks = slab.reshape(2, N_INNER, ROWS_DEV, N_INNER, width)
    return jnp.transpose(blocks, (0, 3, 2, 1, 4)).reshape(2, N_INNER * ROWS_DEV, BRANCH)


def reference(stem_slab, branches, column_order):
    current = stem_slab
    for section_index in range(STEPS):
        if section_index > 0:
            current = swap_blocks(current)
        current = contract(current, column_order[section_index], branches[section_index])
    return current
```

```python
import functools

import jax
import jax.numpy as jnp
from jax import lax
from jax.experimental import pallas as pl
from jax.experimental.pallas import tpu as pltpu
from jax.sharding import PartitionSpec as P


LANES = 128
CHUNKS = 2
F32 = jnp.float32
BF16 = jnp.bfloat16
ANY = pl.BlockSpec(memory_space=pl.ANY)


def add_block(ordered, block_rows):
    real_part = jnp.dot(ordered[0], block_rows[0], preferred_element_type=F32) - jnp.dot(
        ordered[1], block_rows[1], preferred_element_type=F32
    )
    imag_part = jnp.dot(ordered[0], block_rows[1], preferred_element_type=F32) + jnp.dot(
        ordered[1], block_rows[0], preferred_element_type=F32
    )
    return jnp.stack([real_part, imag_part])


def folded(slab, order_row, branch_slice):
    ordered = jnp.take(slab, order_row, axis=2)
    summed = add_block(ordered, lax.all_gather(branch_slice, "inner", axis=1, tiled=True))
    return summed.astype(BF16)


def plain(stem_slab, branches, column_order):
    current = folded(stem_slab, column_order[0], branches[0])
    for section_index in range(1, branches.shape[0]):
        current = lax.all_to_all(current, "inner", split_axis=2, concat_axis=2, tiled=True)
        current = folded(current, column_order[section_index], branches[section_index])
    return current


def wait_all(ref, sem):
    pltpu.make_async_copy(ref, ref, sem).wait()


def product_tile(x_ref, w_ref, lo, width):
    columns = pl.ds(lo, width)
    dot = functools.partial(jnp.dot, preferred_element_type=F32)
    real_in, imag_in = x_ref[0], x_ref[1]
    real_w, imag_w = w_ref[0, :, columns], w_ref[1, :, columns]
    return dot(real_in, real_w) - dot(imag_in, imag_w), dot(real_in, imag_w) + dot(imag_in, real_w)


def reorder(x, pick_ref):
    return jnp.dot(x, pick_ref[...], preferred_element_type=F32).astype(BF16)


def start_branch(places, refs, section, mine, w_ref, sem, q):
    for refs_index, item, half, j in places:
        target = mine if half == 0 else 1 - mine
        pltpu.make_async_copy(
            refs[refs_index].at[item, section], w_ref.at[target, pl.ds(j * q, q)], sem
        ).start()


def mid_kernel(n, q, rc, chunk, places, n_w, scalars, pick0, pick1, *rest):
    pieces, rest = rest[: n // 2], rest[n // 2 :]
    w_refs, rest = rest[:n_w], rest[n_w:]
    own_out, sib_out, x_in, x_now, pick, w0, w1, y_out, sems = rest
    me, mine = scalars[0], scalars[1]
    for kc, piece in enumerate(pieces):
        pltpu.make_async_copy(
            piece.at[:, :, pl.ds(chunk * rc, rc)], x_in.at[:, pl.ds(2 * kc, 2)], sems.at[0]
        ).start()
    pltpu.make_async_copy(pick0, pick.at[0], sems.at[1]).start()
    start_branch(places, w_refs, 0, mine, w0, sems.at[2], q)
    pltpu.make_async_copy(pick1, pick.at[1], sems.at[3]).start()
    start_branch(places, w_refs, 1, mine, w1, sems.at[4], q)

    m, k = x_now.shape[1:]
    low_half = lax.broadcasted_iota(jnp.int32, (rc, LANES), 1) < q
    tile = 2 * LANES

    def swapped(w_ref, store):
        for lo in range(0, k, tile):
            for p, y in enumerate(product_tile(x_now, w_ref, lo, tile)):
                for s in range(0, tile, LANES):
                    part = y[:, s : s + LANES]
                    turned = pltpu.roll(part, q, 1)
                    d = (lo + s) // q
                    for j in range(0, n, 2):
                        even, odd = slice(j * rc, (j + 1) * rc), slice((j + 1) * rc, (j + 2) * rc)
                        store(p, d, j * q, jnp.where(low_half, part[even], turned[odd]).astype(BF16))
                        store(p, d + 1, j * q, jnp.where(low_half, turned[even], part[odd]).astype(BF16))

    wait_all(x_in, sems.at[0])
    wait_all(pick.at[0], sems.at[1])
    for p in range(2):
        x_now[p] = reorder(x_in[p].reshape(m, k), pick.at[0])
    wait_all(w0, sems.at[2])

    def store_mid(p, d, lo, value):
        x_in[p, d, :, lo : lo + LANES] = value

    swapped(w0, store_mid)
    wait_all(pick.at[1], sems.at[3])
    for p in range(2):
        x_now[p] = reorder(x_in[p].reshape(m, k), pick.at[1])
    wait_all(w1, sems.at[4])

    def store_out(p, h, lo, value):
        y_out[h, p, :, lo : lo + LANES] = value

    swapped(w1, store_out)
    for kc in range(n // 2):
        pltpu.make_async_copy(y_out.at[me ^ (2 * kc)], own_out.at[kc], sems.at[5]).start()
        pltpu.make_async_copy(y_out.at[me ^ (2 * kc + 1)], sib_out.at[kc], sems.at[5]).start()
    wait_all(y_out, sems.at[5])


def fin_kernel(n, q, rc, chunk, places, n_w, with_prev, scalars, pick2, *rest):
    pieces, rest = rest[: n // 2], rest[n // 2 :]
    w_refs, rest = rest[:n_w], rest[n_w:]
    if with_prev:
        rest = rest[1:]
    out, x_in, x_now, pick, w2, y_out, sems = rest
    me, mine = scalars[0], scalars[1]
    for kc, piece in enumerate(pieces):
        for cr in range(2):
            for p in range(2):
                pltpu.make_async_copy(piece.at[cr, p], x_in.at[p, 2 * kc + cr], sems.at[0]).start()
    pltpu.make_async_copy(pick2, pick, sems.at[1]).start()
    start_branch(places, w_refs, 0, mine, w2, sems.at[2], q)
    m, k = x_now.shape[1:]
    rows = n * rc // n * CHUNKS
    tile = 2 * LANES
    wait_all(x_in, sems.at[0])
    wait_all(pick, sems.at[1])
    for p in range(2):
        x_now[p] = reorder(x_in[p].reshape(m, k), pick)
    wait_all(w2, sems.at[2])
    for lo in range(0, k, tile):
        for p, y in enumerate(product_tile(x_now, w2, lo, tile)):
            y_out[p, :, :, lo : lo + tile] = y.astype(BF16).reshape(n, rc, tile)
    for j in range(n):
        start = pl.multiple_of((me ^ j) * rows + chunk * rc, rc)
        pltpu.make_async_copy(y_out.at[:, j], out.at[:, pl.ds(start, rc)], sems.at[3]).start()
    wait_all(y_out, sems.at[3])


def flat_cost(flops, size):
    return pl.CostEstimate(flops=flops, bytes_accessed=size, transcendentals=0)


def local(n, stem_slab, branches, column_order):
    chips = n // 2
    rows, k = stem_slab.shape[1:]
    q = k // n
    block = rows // n
    rc = block // CHUNKS
    m = n * rc
    me = lax.axis_index("inner")
    core, chip = me & 1, me >> 1
    n_parts = lax.axis_size("parts")
    mine_index = lax.axis_index("parts") & 1
    scalars = jnp.stack([me, mine_index]).astype(jnp.int32)

    def swap_inner(x, mask):
        return lax.ppermute(x, "inner", [(i, i ^ mask) for i in range(n)])

    def swap_parts(x):
        return lax.ppermute(x, "parts", [(i, i ^ 1) for i in range(n_parts)])

    def gather_branch(pair):
        mine = lax.dynamic_index_in_dim(pair, mine_index, 1, keepdims=False)
        other = lax.dynamic_index_in_dim(pair, 1 - mine_index, 1, keepdims=False)
        top, low = n // 2, n // 4
        near = swap_inner(mine, low)
        far = swap_inner(mine, top | low)
        held = {0: mine, low: near, top | low: far}
        held[top] = swap_inner(far, low)
        first = [low, top | low]
        stages = [first]
        bit = low // 2
        early, late = [0, low], [top, top | low]
        while bit >= 2:
            for group in (early, late):
                got = swap_inner(jnp.stack([held[i] for i in group]), bit)
                for at, i in enumerate(group):
                    held[i | bit] = got[at]
            stages.append(([top] if bit == low // 2 else []) + [i | bit for i in early])
            stages.append([i | bit for i in late])
            early, late = early + [i | bit for i in early], late + [i | bit for i in late]
            bit //= 2
        stacks, places = [], []
        for number, stage in enumerate(stages):
            got = swap_parts(jnp.stack([held[i] for i in stage]))
            items = [(held[i], 0, i) for i in stage] + [(got[at], 1, i) for at, i in enumerate(stage)]
            if number == 0:
                items += [(mine, 0, 0), (other, 1, 0)]
            stack = jnp.stack([item[0] for item in items])
            both = (stack, swap_inner(stack, 1))
            for cr in range(2):
                for at, (_, half, i) in enumerate(items):
                    places.append((len(stacks) + cr, at, half, i + cr))
            stacks += both
        return stacks, tuple(places)

    def chip_exchange(payload_of):
        got = [payload_of(0)] + [None] * (chips - 1)
        for kc in range(chips - 1, 0, -1):
            got[kc] = swap_inner(payload_of(kc), 2 * kc)
        return got

    with jax.named_scope("branch_a"):
        a_stacks, a_places = gather_branch(branches[:2])
    with jax.named_scope("branch_b"):
        b_stacks, b_places = gather_branch(branches[2:])

    relative = jnp.arange(n) ^ me
    order = column_order.reshape(-1, n, q)[:, relative].reshape(-1, k)
    number = lax.broadcasted_iota(jnp.int32, (k, k), 0)

    def one_hot(section, shift):
        return ((number ^ shift) == order[section][None, :]).astype(BF16)

    picks = [one_hot(0, 0), one_hot(1, me * q), one_hot(2, 0)]

    with jax.named_scope("stem_in"):
        by_core = stem_slab.reshape(2, chips, 2, block, k)
        own = lax.dynamic_index_in_dim(by_core, core, 2, keepdims=False)
        sib = swap_inner(lax.dynamic_index_in_dim(by_core, 1 - core, 2, keepdims=False), 1)

        def stem_payload(kc):
            pick = lambda x: lax.dynamic_index_in_dim(x, chip ^ kc, 1, keepdims=False)
            return jnp.stack([pick(own), pick(sib)], axis=1)

        pieces = chip_exchange(stem_payload)

    smem = pl.BlockSpec(memory_space=pltpu.SMEM)
    mm = 8 * m * k * k
    out_shape = jax.ShapeDtypeStruct((chips, 2, rc, k), BF16)

    def mid(chunk):
        return pl.pallas_call(
            functools.partial(mid_kernel, n, q, rc, chunk, a_places, len(a_stacks)),
            out_shape=(out_shape, out_shape),
            in_specs=[smem] + [ANY] * (2 + chips + len(a_stacks)),
            out_specs=(ANY, ANY),
            scratch_shapes=[
                pltpu.VMEM((2, n, rc, k), BF16),
                pltpu.VMEM((2, m, k), BF16),
                pltpu.VMEM((2, k, k), BF16),
                pltpu.VMEM((2, k, k), BF16),
                pltpu.VMEM((2, k, k), BF16),
                pltpu.VMEM((n, 2, rc, k), BF16),
                pltpu.SemaphoreType.DMA((6,)),
            ],
            cost_estimate=flat_cost(3 * mm, 16 * k * k),
            name=f"mid{chunk}",
        )(scalars, picks[0], picks[1], *pieces, *a_stacks)

    def fin(chunk, arrived, prev):
        extra = [] if prev is None else [prev]
        n_in = 2 + chips + len(b_stacks)
        return pl.pallas_call(
            functools.partial(fin_kernel, n, q, rc, chunk, b_places, len(b_stacks), bool(extra)),
            out_shape=jax.ShapeDtypeStruct((2, rows, k), BF16),
            in_specs=[smem] + [ANY] * (n_in - 1 + len(extra)),
            out_specs=ANY,
            scratch_shapes=[
                pltpu.VMEM((2, n, rc, k), BF16),
                pltpu.VMEM((2, m, k), BF16),
                pltpu.VMEM((k, k), BF16),
                pltpu.VMEM((2, k, k), BF16),
                pltpu.VMEM((2, n, rc, k), BF16),
                pltpu.SemaphoreType.DMA((4,)),
            ],
            input_output_aliases={n_in: 0} if extra else {},
            cost_estimate=flat_cost(3 * mm // 2, 8 * k * k),
            name=f"fin{chunk}",
        )(scalars, picks[2], *arrived, *b_stacks, *extra)

    result = None
    for chunk in range(CHUNKS):
        with jax.named_scope(f"stem_out{chunk}"):
            own_out, sib_out = mid(chunk)
            from_sib = swap_inner(sib_out, 1)
            arrived = chip_exchange(lambda kc: jnp.stack([own_out[kc], from_sib[kc]]))
        result = fin(chunk, arrived, result)
    return result


def fits(n, n_parts, rows, k):
    power_of_two = n >= 8 and n & (n - 1) == 0
    return power_of_two and n_parts % 2 == 0 and k == n * LANES // 2 and rows % (n * CHUNKS * 16) == 0


def solution(mesh):
    n, n_parts = mesh.shape["inner"], mesh.shape["parts"]

    def body(stem_slab, branches, column_order):
        if fits(n, n_parts, *stem_slab.shape[1:]):
            return local(n, stem_slab, branches, column_order)
        return plain(stem_slab, branches, column_order)

    in_specs = (P(None, ("parts", "inner"), None), P(None, None, "inner", None), P())
    out_specs = P(None, ("parts", "inner"), None)
    return jax.shard_map(body, mesh=mesh, in_specs=in_specs, out_specs=out_specs, check_vma=False)
```

```python
import functools

import jax
import jax.numpy as jnp
from jax import lax
from jax.experimental import pallas as pl
from jax.experimental.pallas import tpu as pltpu
from jax.sharding import PartitionSpec as P


LANES = 128
CHUNKS = 2
F32 = jnp.float32
BF16 = jnp.bfloat16
ANY = pl.BlockSpec(memory_space=pltpu.HBM)
VMEM = pl.BlockSpec(memory_space=pltpu.VMEM)
ROOM = pltpu.CompilerParams(vmem_limit_bytes=24 * 1024 * 1024)


def add_block(ordered, block_rows):
    real_part = jnp.dot(ordered[0], block_rows[0], preferred_element_type=F32) - jnp.dot(
        ordered[1], block_rows[1], preferred_element_type=F32
    )
    imag_part = jnp.dot(ordered[0], block_rows[1], preferred_element_type=F32) + jnp.dot(
        ordered[1], block_rows[0], preferred_element_type=F32
    )
    return jnp.stack([real_part, imag_part])


def folded(slab, order_row, branch_slice):
    ordered = jnp.take(slab, order_row, axis=2)
    summed = add_block(ordered, lax.all_gather(branch_slice, "inner", axis=1, tiled=True))
    return summed.astype(BF16)


def plain(stem_slab, branches, column_order):
    current = folded(stem_slab, column_order[0], branches[0])
    for section_index in range(1, branches.shape[0]):
        current = lax.all_to_all(current, "inner", split_axis=2, concat_axis=2, tiled=True)
        current = folded(current, column_order[section_index], branches[section_index])
    return current


def wait_all(ref, sem):
    pltpu.make_async_copy(ref, ref, sem).wait()


def branch_tile(places, refs, section, mine, columns):
    rows = {}
    for at, item, half, j, first in places:
        ref = refs[at] if item is None else refs[at].at[item]
        if half is None:
            rows[0, j] = ref[first + section, mine, :, columns]
            rows[1, j] = ref[first + section, 1 - mine, :, columns]
        else:
            rows[half, j] = ref[section, :, columns]
    return [jnp.concatenate([rows[half, j] for j in range(len(rows) // 2)], axis=0) for half in (0, 1)]


def product_tile(x_ref, w_real, w_imag):
    m = x_ref.shape[0] // 2
    by_real = jnp.dot(x_ref[...], w_real, preferred_element_type=F32)
    by_imag = jnp.dot(x_ref[...], w_imag, preferred_element_type=F32)
    return by_real[:m] - by_imag[m:], by_imag[:m] + by_real[m:]


def product_tile_halves(x_ref, w_mine, w_other, mine):
    m = x_ref.shape[0] // 2
    by_mine = jnp.dot(x_ref[...], w_mine, preferred_element_type=F32)
    by_other = jnp.dot(x_ref[...], w_other, preferred_element_type=F32)
    by_real = jnp.where(mine == 0, by_mine, by_other)
    by_imag = jnp.where(mine == 0, by_other, by_mine)
    return by_real[:m] - by_imag[m:], by_imag[:m] + by_real[m:]


def reorder(x_in, pick_ref, x_now):
    rows, k = x_now.shape
    x = x_in[...].reshape(rows, k)
    for lo in range(0, k, 2 * LANES):
        columns = pl.ds(lo, 2 * LANES)
        x_now[:, columns] = jnp.dot(x, pick_ref[:, columns], preferred_element_type=F32).astype(BF16)


def mid_kernel(n, q, rc, chunk, places, n_w, scalars, picks, *rest):
    pieces, rest = rest[: n // 2], rest[n // 2 :]
    w_refs, rest = rest[:n_w], rest[n_w:]
    outs, rest = rest[: n // 2], rest[n // 2 :]
    x_in, x_now, y_out = rest
    me, mine = scalars[0], scalars[1]
    for kc, piece in enumerate(pieces):
        x_in[:, 2 * kc : 2 * kc + 2] = piece[:, :, chunk * rc : (chunk + 1) * rc, :]
    k = x_now.shape[1]
    low_half = lax.broadcasted_iota(jnp.int32, (rc, LANES), 1) < q
    tile = 2 * LANES

    def swapped(section, store):
        for lo in range(0, k, tile):
            halves = branch_tile(places, w_refs, section, mine, pl.ds(lo, tile))
            for p, y in enumerate(product_tile_halves(x_now, *halves, mine)):
                for s in range(0, tile, LANES):
                    part = y[:, s : s + LANES]
                    turned = pltpu.roll(part, q, 1)
                    d = (lo + s) // q
                    for j in range(0, n, 2):
                        even, odd = slice(j * rc, (j + 1) * rc), slice((j + 1) * rc, (j + 2) * rc)
                        store(p, d, j * q, jnp.where(low_half, part[even], turned[odd]).astype(BF16))
                        store(p, d + 1, j * q, jnp.where(low_half, turned[even], part[odd]).astype(BF16))

    reorder(x_in, picks.at[0], x_now)

    def store_mid(p, d, lo, value):
        x_in[p, d, :, lo : lo + LANES] = value

    swapped(0, store_mid)
    reorder(x_in, picks.at[1], x_now)

    def store_out(p, h, lo, value):
        y_out[h, p, :, lo : lo + LANES] = value

    swapped(1, store_out)
    for kc in range(n // 2):
        for cr in range(2):
            outs[kc][cr] = y_out[me ^ (2 * kc + cr)]


def join_kernel(items, *refs):
    parts, (out, held, sems) = refs[:-3], refs[-3:]
    for at, (part, item) in enumerate(items):
        source = parts[part] if item is None else parts[part].at[item]
        pltpu.make_async_copy(source, held.at[at], sems.at[0]).start()
    wait_all(held, sems.at[0])
    put = pltpu.make_async_copy(held, out, sems.at[1])
    put.start()
    put.wait()


def turn_kernel(places, n_w, scalars, picks, *rest):
    w_refs, out = rest[:n_w], rest[n_w]
    mine = scalars[1]
    pick = picks[picks.shape[0] - 1]
    for lo in range(0, out.shape[2], 2 * LANES):
        columns = pl.ds(lo, 2 * LANES)
        for half, w in enumerate(branch_tile(places, w_refs, 0, mine, columns)):
            turned = jnp.dot(pick, w, preferred_element_type=F32).astype(BF16)
            out[mine if half == 0 else 1 - mine, :, columns] = turned


def fin_kernel(n, rc, chunk, with_prev, scalars, branch, *rest):
    pieces, forwarded, rest = rest[: n // 2], rest[n // 2], rest[n // 2 + 1 :]
    if with_prev:
        rest = rest[1:]
    out, x_in, y_out, sems = rest
    me = scalars[0]
    for kc, piece in enumerate(pieces):
        x_in[:, 2 * kc] = piece[0]
        x_in[:, 2 * kc + 1] = forwarded[kc]
    k = x_in.shape[3]
    rows = rc * CHUNKS
    tile = 2 * LANES
    x_now = x_in.reshape(2 * n * rc, k)
    for lo in range(0, k, tile):
        for p, y in enumerate(product_tile(x_now, branch[0, :, lo : lo + tile], branch[1, :, lo : lo + tile])):
            y_out[p, :, :, lo : lo + tile] = y.astype(BF16).reshape(n, rc, tile)
    for j in range(n):
        start = pl.multiple_of((me ^ j) * rows + chunk * rc, rc)
        pltpu.make_async_copy(y_out.at[:, j], out.at[:, pl.ds(start, rc)], sems.at[2]).start()
    wait_all(y_out, sems.at[2])


def pick_kernel(q, scalars, order, out, row):
    me, (sections, rows, k) = scalars[0], out.shape
    step = 2 * LANES
    for section in range(sections):
        for at in range(k // LANES):
            block = order[section, pl.ds(at ^ (me >> 1), 1), :]
            row[:, at * LANES : (at + 1) * LANES] = jnp.where((me & 1) == 1, pltpu.roll(block, q, 1), block)
        shift = me * q if section == 1 else 0
        for lo in range(0, rows, step):
            number = lo + lax.broadcasted_iota(jnp.int32, (step, k), 0)
            out[section, lo : lo + step] = ((number ^ shift) == row[...]).astype(F32).astype(BF16)


def prep_kernel(scalars, stem, sib, x, sem):
    core = scalars[0] & 1
    for copy in (
        pltpu.make_async_copy(stem.at[:, :, 1 - core], x, sem),
        pltpu.make_async_copy(x, sib, sem),
    ):
        copy.start()
        copy.wait()


def pack_kernel(scalars, stem, sib, *rest):
    outs, (x, sems) = rest[:-2], rest[-2:]
    core, chip = scalars[0] & 1, scalars[0] >> 1
    takes = [
        pltpu.make_async_copy(stem.at[:, :, core], x.at[0], sems.at[0]),
        pltpu.make_async_copy(sib, x.at[1], sems.at[1]),
    ]
    for take in takes:
        take.start()
    for take in takes:
        take.wait()
    for kc in reversed(range(len(outs))):
        for cr in range(2):
            pltpu.make_async_copy(x.at[cr, :, chip ^ kc], outs[kc].at[:, cr], sems.at[2]).start()
    wait_all(x, sems.at[2])


def forward_kernel(*refs):
    pieces, (out, blocks, sems) = refs[:-3], refs[-3:]
    for kc, piece in enumerate(pieces):
        pltpu.make_async_copy(piece.at[1], blocks.at[kc], sems.at[0]).start()
    wait_all(blocks, sems.at[0])
    put = pltpu.make_async_copy(blocks, out, sems.at[1])
    put.start()
    put.wait()


def flat_cost(flops, size):
    return pl.CostEstimate(flops=flops, bytes_accessed=size, transcendentals=0)


def local(n, stem_slab, branches, column_order):
    chips = n // 2
    rows, k = stem_slab.shape[1:]
    q = k // n
    block = rows // n
    rc = block // CHUNKS
    m = n * rc
    me = lax.axis_index("inner")
    n_parts = lax.axis_size("parts")
    mine_index = lax.axis_index("parts") & 1
    scalars = jnp.stack([me, mine_index]).astype(jnp.int32)

    def swap_inner(x, mask):
        return lax.ppermute(x, "inner", [(i, i ^ mask) for i in range(n)])

    def swap_parts(x):
        return lax.ppermute(x, "parts", [(i, i ^ 1) for i in range(n_parts)])

    smem = pl.BlockSpec(memory_space=pltpu.SMEM)
    vmem = pltpu.VMEM
    sections = column_order.shape[0]
    split = sections - 1
    by_core = stem_slab.reshape(2, chips, 2, block, k)

    def shape(*dims):
        return jax.ShapeDtypeStruct(dims, BF16)

    for_sib = pl.pallas_call(
        prep_kernel,
        out_shape=shape(2, chips, block, k),
        in_specs=[smem, ANY],
        out_specs=ANY,
        scratch_shapes=[vmem((2, chips, block, k), BF16), pltpu.SemaphoreType.DMA],
        cost_estimate=flat_cost(0, 4 * rows * k),
        compiler_params=ROOM,
        name="prep",
    )(scalars, by_core)

    def joined(parts):
        arrays, items = [], []
        for array, item in parts:
            at = next((i for i, other in enumerate(arrays) if other is array), len(arrays))
            arrays[at:] = [array] if at == len(arrays) else arrays[at:]
            items.append((at, item))
        piece = parts[0][0].shape if parts[0][1] is None else parts[0][0].shape[1:]
        whole = shape(len(parts), *piece)
        return pl.pallas_call(
            functools.partial(join_kernel, tuple(items)),
            out_shape=whole,
            in_specs=[ANY] * len(arrays),
            out_specs=ANY,
            scratch_shapes=[vmem(whole.shape, BF16), pltpu.SemaphoreType.DMA((2,))],
            cost_estimate=flat_cost(0, 4 * whole.size),
            compiler_params=ROOM,
        )(*arrays)

    top, low = n // 2, n // 4
    own_sib = swap_inner(branches, 1)

    def start_gather(first, count):
        mine = lax.dynamic_slice(branches, (first, mine_index, 0, 0), (count, 1, q, k))[:, 0]
        far = swap_inner(mine, top | low)
        near = swap_inner(mine, low)
        held = {0: (mine, None), low: (near, None), top | low: (far, None)}
        held[top] = (swap_inner(far, low), None)
        return held

    def finish_gather(held, others, groups, first):
        sources, places = [], []

        def place(value, j, half):
            array, item = value
            at = next((i for i, other in enumerate(sources) if other is array), len(sources))
            sources[at:] = [array] if at == len(sources) else sources[at:]
            places.append((at, item, half, j))

        for group in groups:
            parts = [(held[i], 0, i) for i in group] + [(others[i], 1, i) for i in group]
            got = swap_inner(joined([part[0] for part in parts]), 1)
            for at, (value, half, i) in enumerate(parts):
                place(value, i, half)
                place((got, at), i + 1, half)
        places += [(len(sources), None, None, 0), (len(sources) + 1, None, None, 1)]
        sources += [branches, own_sib]
        shifted = [(at, item, half, j, first if half is None else 0) for at, item, half, j in places]
        return sources, tuple(shifted)

    def gather_by_piece(first, count):
        held = start_gather(first, count)
        bit = low // 2
        while bit >= 2:
            for i in list(held):
                held[i | bit] = (swap_inner(held[i][0], bit), None)
            bit //= 2
        others = {i: (swap_parts(held[i][0]), None) for i in held if i}
        last = [i for i in held if i & 2 and i & top]
        early = [i for i in held if i and i not in last]
        return finish_gather(held, others, [early, last], first)

    def gather_joined(first, count):
        held = start_gather(first, count)
        bit = low // 2
        while bit >= 2:
            now = list(held)
            got = swap_inner(joined([held[i] for i in now]), bit)
            held.update({i | bit: (got, at) for at, i in enumerate(now)})
            bit //= 2
        rest = [i for i in held if i]
        got = swap_parts(joined([held[i] for i in rest]))
        others = {i: (got, at) for at, i in enumerate(rest)}
        return finish_gather(held, others, [rest], first)

    def chip_exchange(payloads):
        got = [payloads[0]] + [None] * (chips - 1)
        for kc in range(chips - 1, 0, -1):
            got[kc] = swap_inner(payloads[kc], 2 * kc)
        return got

    a_stacks, a_places = gather_by_piece(0, split)
    b_stacks, b_places = gather_joined(split, sections - split)

    picks = pl.pallas_call(
        functools.partial(pick_kernel, q),
        out_shape=shape(sections, k, k),
        in_specs=[smem, VMEM],
        out_specs=VMEM,
        scratch_shapes=[vmem((1, k), jnp.int32)],
        compiler_params=ROOM,
        cost_estimate=flat_cost(0, 2 * sections * k * k),
        name="picks",
    )(scalars, column_order.reshape(sections, k // LANES, LANES))

    from_sib = swap_inner(for_sib, 1)
    payloads = pl.pallas_call(
        pack_kernel,
        out_shape=[shape(2, 2, block, k)] * chips,
        in_specs=[smem, ANY, ANY],
        out_specs=[ANY] * chips,
        scratch_shapes=[vmem((2, 2, chips, block, k), BF16), pltpu.SemaphoreType.DMA((3,))],
        cost_estimate=flat_cost(0, 8 * rows * k),
        compiler_params=ROOM,
        name="pack",
    )(scalars, by_core, from_sib)
    pieces = chip_exchange(payloads)

    mm = 8 * m * k * k

    def mid(chunk):
        return pl.pallas_call(
            functools.partial(mid_kernel, n, q, rc, chunk, a_places, len(a_stacks)),
            out_shape=[shape(2, 2, rc, k)] * chips,
            in_specs=[smem] + [VMEM] * (1 + chips + len(a_stacks)),
            out_specs=[VMEM] * chips,
            scratch_shapes=[
                pltpu.VMEM((2, n, rc, k), BF16),
                pltpu.VMEM((2 * m, k), BF16),
                pltpu.VMEM((n, 2, rc, k), BF16),
            ],
            cost_estimate=flat_cost(3 * mm, 16 * k * k),
            compiler_params=ROOM,
        )(scalars, picks, *pieces, *a_stacks)

    branch = pl.pallas_call(
        functools.partial(turn_kernel, b_places, len(b_stacks)),
        out_shape=shape(2, k, k),
        in_specs=[smem] + [VMEM] * (1 + len(b_stacks)),
        out_specs=VMEM,
        cost_estimate=flat_cost(4 * k * k * k, 8 * k * k),
        compiler_params=ROOM,
        name="turn",
    )(scalars, picks, *b_stacks)

    def fin(chunk, arrived, prev):
        extra = [] if prev is None else [prev]
        n_in = 3 + chips
        return pl.pallas_call(
            functools.partial(fin_kernel, n, rc, chunk, bool(extra)),
            out_shape=shape(2, rows, k),
            in_specs=[smem] + [VMEM] * (n_in - 1) + [ANY] * len(extra),
            out_specs=ANY,
            scratch_shapes=[
                vmem((2, n, rc, k), BF16),
                vmem((2, n, rc, k), BF16),
                pltpu.SemaphoreType.DMA((3,)),
            ],
            input_output_aliases={n_in: 0} if extra else {},
            cost_estimate=flat_cost(mm, 8 * k * k),
            compiler_params=ROOM,
        )(scalars, branch, *arrived, *extra)

    result = None
    for chunk in range(CHUNKS):
        outs = mid(chunk)
        arrived = chip_exchange(outs)
        forwarded = pl.pallas_call(
            forward_kernel,
            out_shape=shape(chips, 2, rc, k),
            in_specs=[ANY] * chips,
            out_specs=ANY,
            scratch_shapes=[vmem((chips, 2, rc, k), BF16), pltpu.SemaphoreType.DMA((2,))],
            cost_estimate=flat_cost(0, 8 * m * k),
            compiler_params=ROOM,
        )(*arrived)
        arrived = arrived + [swap_inner(forwarded, 1)]
        result = fin(chunk, arrived, result)
    return result


def fits(n, n_parts, rows, k):
    power_of_two = n >= 8 and n & (n - 1) == 0
    return power_of_two and n_parts % 2 == 0 and k == n * LANES // 2 and rows % (n * CHUNKS * 16) == 0


def solution(mesh):
    n, n_parts = mesh.shape["inner"], mesh.shape["parts"]

    def body(stem_slab, branches, column_order):
        if not fits(n, n_parts, *stem_slab.shape[1:]):
            return plain(stem_slab, branches, column_order)
        return local(n, stem_slab, branches, column_order)

    in_specs = (P(None, ("parts", "inner"), None), P(None, None, "inner", None), P())
    out_specs = P(None, ("parts", "inner"), None)
    return jax.shard_map(body, mesh=mesh, in_specs=in_specs, out_specs=out_specs, check_vma=False)
```

```python
import functools

import jax
import jax.numpy as jnp
from jax import lax
from jax.experimental import pallas as pl
from jax.experimental.pallas import tpu as pltpu
from jax.sharding import PartitionSpec as P


LANES = 128
CHUNKS = 2
F32 = jnp.float32
BF16 = jnp.bfloat16
ANY = pl.BlockSpec(memory_space=pltpu.HBM)
VMEM = pl.BlockSpec(memory_space=pltpu.VMEM)
ROOM = pltpu.CompilerParams(vmem_limit_bytes=24 * 1024 * 1024)


def add_block(ordered, block_rows):
    real_part = jnp.dot(ordered[0], block_rows[0], preferred_element_type=F32) - jnp.dot(
        ordered[1], block_rows[1], preferred_element_type=F32
    )
    imag_part = jnp.dot(ordered[0], block_rows[1], preferred_element_type=F32) + jnp.dot(
        ordered[1], block_rows[0], preferred_element_type=F32
    )
    return jnp.stack([real_part, imag_part])


def folded(slab, order_row, branch_slice):
    ordered = jnp.take(slab, order_row, axis=2)
    summed = add_block(ordered, lax.all_gather(branch_slice, "inner", axis=1, tiled=True))
    return summed.astype(BF16)


def plain(stem_slab, branches, column_order):
    current = folded(stem_slab, column_order[0], branches[0])
    for section_index in range(1, branches.shape[0]):
        current = lax.all_to_all(current, "inner", split_axis=2, concat_axis=2, tiled=True)
        current = folded(current, column_order[section_index], branches[section_index])
    return current


def wait_all(ref, sem):
    pltpu.make_async_copy(ref, ref, sem).wait()


def branch_rows(places, refs, section, mine, columns, half):
    rows = {}
    for at, item, own_half, j, first in places:
        ref = refs[at] if item is None else refs[at].at[item]
        if own_half is None:
            rows[j] = ref[first + section, 1 - mine if half else mine, :, columns]
        elif own_half == half:
            rows[j] = ref[section, :, columns]
    return jnp.concatenate([rows[j] for j in range(len(rows))], axis=0)


def product_tile(x_ref, w_mine, w_other, mine):
    m = x_ref.shape[0] // 2
    by_mine = jnp.dot(x_ref[...], w_mine, preferred_element_type=F32)
    by_other = jnp.dot(x_ref[...], w_other, preferred_element_type=F32)
    by_real = jnp.where(mine == 0, by_mine, by_other)
    by_imag = jnp.where(mine == 0, by_other, by_mine)
    return by_real[:m] - by_imag[m:], by_imag[:m] + by_real[m:]


def reorder(x_in, pick_ref, x_now):
    rows, k = x_now.shape
    x = x_in[...].reshape(rows, k)
    for lo in range(0, k, 2 * LANES):
        columns = pl.ds(lo, 2 * LANES)
        x_now[:, columns] = jnp.dot(x, pick_ref[:, columns], preferred_element_type=F32).astype(BF16)


def mid_kernel(n, q, rc, chunk, places, n_w, scalars, picks, *rest):
    pieces, rest = rest[: n // 2], rest[n // 2 :]
    w_refs, rest = rest[:n_w], rest[n_w:]
    outs, rest = rest[: n // 2], rest[n // 2 :]
    x_in, x_now, y_out = rest
    me, mine = scalars[0], scalars[1]
    for kc, piece in enumerate(pieces):
        lo = chunk * rc if piece.shape[2] > rc else 0
        x_in[:, 2 * kc : 2 * kc + 2] = piece[:, :, lo : lo + rc, :]
    k = x_now.shape[1]
    low_half = lax.broadcasted_iota(jnp.int32, (rc, LANES), 1) < q
    tile = 2 * LANES

    def swapped(section, store):
        for lo in range(0, k, tile):
            halves = [branch_rows(places, w_refs, section, mine, pl.ds(lo, tile), half) for half in (0, 1)]
            for p, y in enumerate(product_tile(x_now, *halves, mine)):
                for s in range(0, tile, LANES):
                    part = y[:, s : s + LANES]
                    turned = pltpu.roll(part, q, 1)
                    d = (lo + s) // q
                    for j in range(0, n, 2):
                        even, odd = slice(j * rc, (j + 1) * rc), slice((j + 1) * rc, (j + 2) * rc)
                        store(p, d, j * q, jnp.where(low_half, part[even], turned[odd]).astype(BF16))
                        store(p, d + 1, j * q, jnp.where(low_half, turned[even], part[odd]).astype(BF16))

    reorder(x_in, picks.at[0], x_now)

    def store_mid(p, d, lo, value):
        x_in[p, d, :, lo : lo + LANES] = value

    swapped(0, store_mid)
    reorder(x_in, picks.at[1], x_now)

    def store_out(p, h, lo, value):
        y_out[h, p, :, lo : lo + LANES] = value

    swapped(1, store_out)
    for kc in range(n // 2):
        for cr in range(2):
            outs[kc][cr] = y_out[me ^ (2 * kc + cr)]


def join_kernel(items, *refs):
    parts, (out, held, sems) = refs[:-3], refs[-3:]
    for at, (part, item) in enumerate(items):
        source = parts[part] if item is None else parts[part].at[item]
        pltpu.make_async_copy(source, held.at[at], sems.at[0]).start()
    wait_all(held, sems.at[0])
    put = pltpu.make_async_copy(held, out, sems.at[1])
    put.start()
    put.wait()


def turn_kernel(places, half, scalars, picks, *rest):
    w_refs, out = rest[:-1], rest[-1]
    pick = picks[picks.shape[0] - 1]
    for lo in range(0, out.shape[1], 2 * LANES):
        columns = pl.ds(lo, 2 * LANES)
        w = branch_rows(places, w_refs, 0, scalars[1], columns, half)
        out[:, columns] = jnp.dot(pick, w, preferred_element_type=F32).astype(BF16)


def fin_kernel(n, rc, chunk, with_prev, scalars, w_mine, w_other, *rest):
    pieces, forwarded, rest = rest[: n // 2], rest[n // 2], rest[n // 2 + 1 :]
    if with_prev:
        rest = rest[1:]
    out, x_in, y_out, sems = rest
    me = scalars[0]
    for kc, piece in enumerate(pieces):
        x_in[:, 2 * kc] = piece[0]
        x_in[:, 2 * kc + 1] = forwarded[kc]
    k = x_in.shape[3]
    rows = rc * CHUNKS
    tile = 2 * LANES
    x_now = x_in.reshape(2 * n * rc, k)
    for lo in range(0, k, tile):
        for p, y in enumerate(product_tile(x_now, w_mine[:, lo : lo + tile], w_other[:, lo : lo + tile], scalars[1])):
            y_out[p, :, :, lo : lo + tile] = y.astype(BF16).reshape(n, rc, tile)
    for j in range(n):
        start = pl.multiple_of((me ^ j) * rows + chunk * rc, rc)
        pltpu.make_async_copy(y_out.at[:, j], out.at[:, pl.ds(start, rc)], sems.at[2]).start()
    wait_all(y_out, sems.at[2])


def pick_kernel(q, scalars, order, out, row):
    me, (sections, rows, k) = scalars[0], out.shape
    step = 2 * LANES
    for section in range(sections):
        for at in range(k // LANES):
            block = order[section, pl.ds(at ^ (me >> 1), 1), :]
            row[:, at * LANES : (at + 1) * LANES] = jnp.where((me & 1) == 1, pltpu.roll(block, q, 1), block)
        shift = me * q if section == 1 else 0
        for lo in range(0, rows, step):
            number = lo + lax.broadcasted_iota(jnp.int32, (step, k), 0)
            out[section, lo : lo + step] = ((number ^ shift) == row[...]).astype(F32).astype(BF16)


def prep_kernel(scalars, stem, sib, x, sem):
    core = scalars[0] & 1
    for copy in (
        pltpu.make_async_copy(stem.at[:, :, 1 - core], x, sem),
        pltpu.make_async_copy(x, sib, sem),
    ):
        copy.start()
        copy.wait()


def pack_kernel(plan, scalars, stem, sib, *rest):
    outs, (x, sems) = rest[:-2], rest[-2:]
    core, chip = scalars[0] & 1, scalars[0] >> 1
    takes = [
        pltpu.make_async_copy(stem.at[:, :, core], x.at[0], sems.at[0]),
        pltpu.make_async_copy(sib, x.at[1], sems.at[1]),
    ]
    for take in takes:
        take.start()
    for take in takes:
        take.wait()
    for out, (kc, lo) in zip(outs, plan):
        for cr in range(2):
            source = x.at[cr, :, chip ^ kc, pl.ds(lo, out.shape[2])]
            pltpu.make_async_copy(source, out.at[:, cr], sems.at[2]).start()
    wait_all(x, sems.at[2])


def forward_kernel(*refs):
    pieces, (out, blocks, sems) = refs[:-3], refs[-3:]
    for kc, piece in enumerate(pieces):
        pltpu.make_async_copy(piece.at[1], blocks.at[kc], sems.at[0]).start()
    wait_all(blocks, sems.at[0])
    put = pltpu.make_async_copy(blocks, out, sems.at[1])
    put.start()
    put.wait()


def flat_cost(flops, size):
    return pl.CostEstimate(flops=flops, bytes_accessed=size, transcendentals=0)


def local(n, stem_slab, branches, column_order):
    chips = n // 2
    rows, k = stem_slab.shape[1:]
    q = k // n
    block = rows // n
    rc = block // CHUNKS
    m = n * rc
    me = lax.axis_index("inner")
    n_parts = lax.axis_size("parts")
    mine_index = lax.axis_index("parts") & 1
    scalars = jnp.stack([me, mine_index]).astype(jnp.int32)

    def swap_inner(x, mask):
        return lax.ppermute(x, "inner", [(i, i ^ mask) for i in range(n)])

    def swap_parts(x):
        return lax.ppermute(x, "parts", [(i, i ^ 1) for i in range(n_parts)])

    smem = pl.BlockSpec(memory_space=pltpu.SMEM)
    vmem = pltpu.VMEM
    sections = column_order.shape[0]
    split = sections - 1
    by_core = stem_slab.reshape(2, chips, 2, block, k)

    def shape(*dims):
        return jax.ShapeDtypeStruct(dims, BF16)

    for_sib = pl.pallas_call(
        prep_kernel,
        out_shape=shape(2, chips, block, k),
        in_specs=[smem, ANY],
        out_specs=ANY,
        scratch_shapes=[vmem((2, chips, block, k), BF16), pltpu.SemaphoreType.DMA],
        cost_estimate=flat_cost(0, 4 * rows * k),
        compiler_params=ROOM,
        name="prep",
    )(scalars, by_core)

    def joined(parts):
        arrays, items = [], []
        for array, item in parts:
            at = next((i for i, other in enumerate(arrays) if other is array), len(arrays))
            arrays[at:] = [array] if at == len(arrays) else arrays[at:]
            items.append((at, item))
        piece = parts[0][0].shape if parts[0][1] is None else parts[0][0].shape[1:]
        whole = shape(len(parts), *piece)
        return pl.pallas_call(
            functools.partial(join_kernel, tuple(items)),
            out_shape=whole,
            in_specs=[ANY] * len(arrays),
            out_specs=ANY,
            scratch_shapes=[vmem(whole.shape, BF16), pltpu.SemaphoreType.DMA((2,))],
            cost_estimate=flat_cost(0, 4 * whole.size),
            compiler_params=ROOM,
        )(*arrays)

    top, low = n // 2, n // 4
    own_sib = swap_inner(branches, 1)

    def own_half(first, count, part):
        return lax.dynamic_slice(branches, (first, part, 0, 0), (count, 1, q, k))[:, 0]

    def start_gather(first, count):
        mine = own_half(first, count, mine_index)
        far = swap_inner(mine, top | low)
        near = swap_inner(mine, low)
        held = {0: (mine, None), low: (near, None), top | low: (far, None)}
        held[top] = (swap_inner(far, low), None)
        return held

    def finish_gather(groups, first):
        sources, places = [], []

        def place(value, half, j):
            array, item = value
            at = next((i for i, other in enumerate(sources) if other is array), len(sources))
            sources[at:] = [array] if at == len(sources) else sources[at:]
            places.append((at, item, half, j, 0))

        for group in groups:
            got = swap_inner(joined([value for value, _, _ in group]), 1)
            for at, (value, half, i) in enumerate(group):
                place(value, half, i)
                place((got, at), half, i + 1)
        for j, array in enumerate((branches, own_sib)):
            places.append((len(sources), None, None, j, first))
            sources.append(array)
        return sources, tuple(places)

    def gather_by_piece(first, count):
        held = start_gather(first, count)
        bit = low // 2
        while bit >= 2:
            for i in list(held):
                held[i | bit] = (swap_inner(held[i][0], bit), None)
            bit //= 2
        other = own_half(first, count, 1 - mine_index)
        others = {i: (swap_inner(other, i), None) for i in (low, 2)}
        rest = [i for i in held if i]
        for i in rest:
            if i not in others:
                others[i] = (swap_parts(held[i][0]), None)
        last = [i for i in rest if i & 2 and i & top]
        early = [i for i in rest if i not in last]
        groups = [[(held[i], 0, i) for i in part] + [(others[i], 1, i) for i in part] for part in (early, last)]
        return finish_gather(groups, first)

    def gather_joined(first, count):
        held = start_gather(first, count)
        bit = low // 2
        while bit >= 2:
            now = list(held)
            got = swap_inner(joined([held[i] for i in now]), bit)
            held.update({i | bit: (got, at) for at, i in enumerate(now)})
            bit //= 2
        rest = [i for i in held if i]
        got = swap_parts(joined([held[i] for i in rest]))
        groups = [[(held[i], 0, i) for i in rest], [((got, at), 1, i) for at, i in enumerate(rest)]]
        return finish_gather(groups, first)

    def chip_exchange(payloads):
        got = [payloads[0]] + [None] * (chips - 1)
        for kc in range(chips - 1, 0, -1):
            got[kc] = swap_inner(payloads[kc], 2 * kc)
        return got

    a_stacks, a_places = gather_by_piece(0, split)
    b_stacks, b_places = gather_joined(split, sections - split)

    picks = pl.pallas_call(
        functools.partial(pick_kernel, q),
        out_shape=shape(sections, k, k),
        in_specs=[smem, VMEM],
        out_specs=VMEM,
        scratch_shapes=[vmem((1, k), jnp.int32)],
        compiler_params=ROOM,
        cost_estimate=flat_cost(0, 2 * sections * k * k),
        name="picks",
    )(scalars, column_order.reshape(sections, k // LANES, LANES))

    from_sib = swap_inner(for_sib, 1)
    plan = [(kc, chunk * rc, rc) for kc in range(chips) for chunk in range(CHUNKS)]
    payloads = pl.pallas_call(
        functools.partial(pack_kernel, tuple(entry[:2] for entry in plan)),
        out_shape=[shape(2, 2, size, k) for _, _, size in plan],
        in_specs=[smem, ANY, ANY],
        out_specs=[ANY] * len(plan),
        scratch_shapes=[vmem((2, 2, chips, block, k), BF16), pltpu.SemaphoreType.DMA((3,))],
        cost_estimate=flat_cost(0, 8 * rows * k),
        compiler_params=ROOM,
        name="pack",
    )(scalars, by_core, from_sib)
    pieces = [[None] * chips for _ in range(CHUNKS)]
    for payload, (kc, lo, size) in zip(payloads, plan):
        chunk = lo // rc
        got = swap_inner(payload, 2 * kc) if kc else payload
        for number in range(chunk, chunk + size // rc):
            pieces[number][kc] = got

    mm = 8 * m * k * k

    def mid(chunk):
        return pl.pallas_call(
            functools.partial(mid_kernel, n, q, rc, chunk, a_places, len(a_stacks)),
            out_shape=[shape(2, 2, rc, k)] * chips,
            in_specs=[smem] + [VMEM] * (1 + chips + len(a_stacks)),
            out_specs=[VMEM] * chips,
            scratch_shapes=[
                pltpu.VMEM((2, n, rc, k), BF16),
                pltpu.VMEM((2 * m, k), BF16),
                pltpu.VMEM((n, 2, rc, k), BF16),
            ],
            cost_estimate=flat_cost(3 * mm, 16 * k * k),
            compiler_params=ROOM,
        )(scalars, picks, *pieces[chunk], *a_stacks)

    def turn(half):
        used = [place for place in b_places if place[2] in (None, half)]
        numbers = sorted({place[0] for place in used})
        used = tuple((numbers.index(place[0]),) + place[1:] for place in used)
        return pl.pallas_call(
            functools.partial(turn_kernel, used, half),
            out_shape=shape(k, k),
            in_specs=[smem] + [VMEM] * (1 + len(numbers)),
            out_specs=VMEM,
            cost_estimate=flat_cost(2 * k * k * k, 4 * k * k),
            compiler_params=ROOM,
        )(scalars, picks, *[b_stacks[at] for at in numbers])

    turned = [turn(0), turn(1)]

    def fin(chunk, arrived, prev):
        extra = [] if prev is None else [prev]
        n_in = 4 + chips
        return pl.pallas_call(
            functools.partial(fin_kernel, n, rc, chunk, bool(extra)),
            out_shape=shape(2, rows, k),
            in_specs=[smem] + [VMEM] * (n_in - 1) + [ANY] * len(extra),
            out_specs=ANY,
            scratch_shapes=[
                vmem((2, n, rc, k), BF16),
                vmem((2, n, rc, k), BF16),
                pltpu.SemaphoreType.DMA((3,)),
            ],
            input_output_aliases={n_in: 0} if extra else {},
            cost_estimate=flat_cost(mm, 8 * k * k),
            compiler_params=ROOM,
        )(scalars, *turned, *arrived, *extra)

    result = None
    for chunk in range(CHUNKS):
        outs = mid(chunk)
        arrived = chip_exchange(outs)
        forwarded = pl.pallas_call(
            forward_kernel,
            out_shape=shape(chips, 2, rc, k),
            in_specs=[ANY] * chips,
            out_specs=ANY,
            scratch_shapes=[vmem((chips, 2, rc, k), BF16), pltpu.SemaphoreType.DMA((2,))],
            cost_estimate=flat_cost(0, 8 * m * k),
            compiler_params=ROOM,
        )(*arrived)
        arrived = arrived + [swap_inner(forwarded, 1)]
        result = fin(chunk, arrived, result)
    return result


def fits(n, n_parts, rows, k):
    power_of_two = n >= 8 and n & (n - 1) == 0
    return power_of_two and n_parts % 2 == 0 and k == n * LANES // 2 and rows % (n * CHUNKS * 16) == 0


def solution(mesh):
    n, n_parts = mesh.shape["inner"], mesh.shape["parts"]

    def body(stem_slab, branches, column_order):
        if not fits(n, n_parts, *stem_slab.shape[1:]):
            return plain(stem_slab, branches, column_order)
        return local(n, stem_slab, branches, column_order)

    in_specs = (P(None, ("parts", "inner"), None), P(None, None, "inner", None), P())
    out_specs = P(None, ("parts", "inner"), None)
    return jax.shard_map(body, mesh=mesh, in_specs=in_specs, out_specs=out_specs, check_vma=False)
```
